32 devices in a mesh: gx: 2 (over y), gy: 4 (over x, core), gz: 4 (over z).
Axes of the slice: x: 2, y: 2, z: 4, core: 2. Of those that a mesh axis runs over, the one named last changes fastest.
Arguments:
- node_latents: bfloat16 [32768, 128], P(('gx', 'gy', 'gz')), may hold values from -300 to 300
- cluster_latents: bfloat16 [8192, 128], P(('gx', 'gy', 'gz')), may hold values from -6 to 6
- senders: int32 [1024, 128], P(('gx', 'gy', 'gz')), may hold values from 0 to 4095
- membership: int32 [32768], P(('gx', 'gy', 'gz')), may hold values from 0 to 255
- w_key: bfloat16 [128, 128], replicated, may hold values from -1 to 1
- w_value: bfloat16 [128, 128], replicated, may hold values from -0.5 to 0.5
- w_edge_in: bfloat16 [256, 128], replicated, may hold values from -0.375 to 0.375
- w_edge_out: bfloat16 [128, 128], replicated, may hold values from -0.5 to 0.5
- w_node_in: bfloat16 [512, 128], replicated, may hold values from -0.25 to 0.25
- w_node_out: bfloat16 [128, 128], replicated, may hold values from -0.5 to 0.5
- out_gain: float32 [128], replicated, may hold values from 0.5 to 1.5
Outputs:
- new_latents: bfloat16 [32768, 128], P(('gx', 'gy', 'gz'))
The draws below stay inside these ranges and needn't reach their ends.
All inputs are finite; a program needn't handle non-finite values.
Results may differ from the reference program's by a relative error of at most 0.005.
Values may be sent and summed in bfloat16 or wider, within the bound.
A program may use at most 64 MiB of HBM per device.

```python
import jax
import jax.numpy as jnp
from jax import lax

H = 128
NODES_DEV = 1024
CL_DEV = 256
BND = 512
DEG = 4
EDGE_ROWS = 32
NODES = 32768
CLUSTERS = 8192
N_GX = 2
N_GY = 4
N_GZ = 4
DEVICES = 32


def shared_parts(key):
    cluster_key, weight_key = jax.random.split(jax.random.fold_in(key, 7))
    clusters = jnp.clip(jax.random.normal(cluster_key, (CLUSTERS, H), jnp.float32), -6.0, 6.0)
    weights = jnp.clip(jax.random.normal(weight_key, (H, H), jnp.float32), -6.0, 6.0) / jnp.sqrt(jnp.float32(H))
    return (clusters, weights)


def draw_cluster_latents(key, part):
    return shared_parts(key)[0].astype(jnp.bfloat16)


def draw_w_key(key, part):
    return shared_parts(key)[1].astype(jnp.bfloat16)


def draw_node_latents(key, part):
    base_key = jax.random.fold_in(key, 11)
    latents = jnp.clip(jax.random.normal(base_key, (NODES, H), jnp.float32), -6.0, 6.0)
    return latents.astype(jnp.bfloat16)


def plant(drawn, own_key, least, top_value):
    longest = drawn.shape.index(max(drawn.shape))
    spots = []
    for shift in (0, 1):
        where = [jax.random.randint(jax.random.fold_in(own_key, axis), (), 0, length) for axis, length in enumerate(drawn.shape)]
        where[longest] = (where[longest] + shift) % drawn.shape[longest]
        spots.append(tuple(where))
    return drawn.at[spots[0]].set(least).at[spots[1]].set(top_value)


def normal_values(rng, shape, scale, bound, kind=jnp.bfloat16):
    return jnp.clip(scale * jax.random.normal(rng, shape, jnp.float32), -bound, bound).astype(kind)


def setup_inputs(seed: int = 0) -> dict:
    splits = jax.random.split(jax.random.key(seed), 12)
    node_latents = draw_node_latents(jax.random.fold_in(splits[11], 71), 0)
    cluster_latents = draw_cluster_latents(jax.random.fold_in(splits[11], 71), 0)
    senders = plant(jax.random.randint(splits[2], (DEVICES * EDGE_ROWS, 128), 0, NODES_DEV + 6 * BND), jax.random.fold_in(splits[2], 1), 0, (NODES_DEV + 6 * BND) - 1).astype(jnp.int32)
    membership = plant(jax.random.randint(splits[3], (NODES,), 0, CL_DEV), jax.random.fold_in(splits[3], 1), 0, CL_DEV - 1).astype(jnp.int32)
    w_key = draw_w_key(jax.random.fold_in(splits[11], 71), 0)
    w_value = normal_values(splits[5], (H, H), H ** -0.5, 0.5)
    w_edge_in = normal_values(splits[6], (2 * H, H), (2 * H) ** -0.5, 0.375)
    w_edge_out = normal_values(splits[7], (H, H), H ** -0.5, 0.5)
    w_node_in = normal_values(splits[8], (4 * H, H), (4 * H) ** -0.5, 0.25)
    w_node_out = normal_values(splits[9], (H, H), H ** -0.5, 0.5)
    out_gain = jnp.clip(1.0 + 0.1 * jax.random.normal(splits[10], (H,), jnp.float32), 0.5, 1.5)
    return dict(node_latents=node_latents, cluster_latents=cluster_latents, senders=senders, membership=membership, w_key=w_key, w_value=w_value, w_edge_in=w_edge_in, w_edge_out=w_edge_out, w_node_in=w_node_in, w_node_out=w_node_out, out_gain=out_gain)


def project(latent_rows, weight):
    return jnp.dot(latent_rows, weight, preferred_element_type=jnp.float32).astype(jnp.bfloat16)

def attend(queries, key_rows, value_rows):
    scores = jnp.dot(queries, key_rows.T, preferred_element_type=jnp.float32) / jnp.sqrt(jnp.float32(queries.shape[1]))
    highest = lax.optimization_barrier(jnp.max(scores, axis=1, keepdims=True))
    exponent = jnp.exp(scores - highest)
    numer = jnp.dot(exponent.astype(jnp.bfloat16), value_rows, preferred_element_type=jnp.float32)
    return numer / lax.optimization_barrier(jnp.sum(exponent, axis=1, keepdims=True))

def reference(node_latents, cluster_latents, senders, membership, w_key, w_value, w_edge_in, w_edge_out, w_node_in, w_node_out, out_gain):
    width = node_latents.shape[1]
    key_grid = project(cluster_latents, w_key).reshape(N_GX, N_GY, N_GZ, CL_DEV, width)
    value_grid = project(cluster_latents, w_value).reshape(N_GX, N_GY, N_GZ, CL_DEV, width)
    cluster_grid = cluster_latents.reshape(N_GX, N_GY, N_GZ, CL_DEV, width)
    node_grid = node_latents.reshape(N_GX, N_GY, N_GZ, NODES_DEV, width)
    border = node_grid[:, :, :, :BND]
    faces = jnp.stack([jnp.roll(border, 1, axis=0), jnp.roll(border, -1, axis=0), jnp.roll(border, 1, axis=1), jnp.roll(border, -1, axis=1), jnp.roll(border, 1, axis=2), jnp.roll(border, -1, axis=2)], axis=3)
    faces = faces.reshape(N_GX, N_GY, N_GZ, 6 * BND, width)
    edge_grid = senders.reshape(N_GX, N_GY, N_GZ, NODES_DEV * DEG)
    member_grid = membership.reshape(N_GX, N_GY, N_GZ, NODES_DEV)

    def one_block(device_flat):
        index_x = device_flat // (N_GY * N_GZ)
        index_y = device_flat // N_GZ % N_GY
        index_z = device_flat % N_GZ
        own = node_grid[index_x, index_y, index_z]
        pooled = attend(own, key_grid[:, index_y, index_z].reshape(-1, width), value_grid[:, index_y, index_z].reshape(-1, width))
        pooled = pooled + attend(own, key_grid[index_x, :, index_z].reshape(-1, width), value_grid[index_x, :, index_z].reshape(-1, width))
        pooled = pooled + attend(own, key_grid[index_x, index_y].reshape(-1, width), value_grid[index_x, index_y].reshape(-1, width))
        attended = (pooled * lax.rsqrt(lax.optimization_barrier(jnp.mean(pooled * pooled, axis=1, keepdims=True)) + 1e-06)).astype(jnp.bfloat16)
        extended = jnp.concatenate([own, faces[index_x, index_y, index_z]], axis=0)
        sender_rows = jnp.take(extended, edge_grid[index_x, index_y, index_z], axis=0)
        receiver_part = jnp.dot(own, w_edge_in[:width], preferred_element_type=jnp.float32)
        sender_part = jnp.dot(sender_rows, w_edge_in[width:], preferred_element_type=jnp.float32)
        edge_hidden = jax.nn.silu(sender_part.reshape(NODES_DEV, DEG, width) + receiver_part[:, None, :]).astype(jnp.bfloat16)
        messages = jnp.dot(edge_hidden.reshape(NODES_DEV * DEG, width), w_edge_out, preferred_element_type=jnp.float32)
        aggregated = lax.optimization_barrier(jnp.sum(messages.reshape(NODES_DEV, DEG, width), axis=1)).astype(jnp.bfloat16)
        own_cluster = jnp.take(cluster_grid[index_x, index_y, index_z], member_grid[index_x, index_y, index_z], axis=0)
        preact = jnp.dot(own, w_node_in[:width], preferred_element_type=jnp.float32)
        preact = preact + jnp.dot(aggregated, w_node_in[width:2 * width], preferred_element_type=jnp.float32)
        preact = preact + jnp.dot(attended, w_node_in[2 * width:3 * width], preferred_element_type=jnp.float32)
        preact = preact + jnp.dot(own_cluster, w_node_in[3 * width:], preferred_element_type=jnp.float32)
        node_hidden = jax.nn.silu(preact).astype(jnp.bfloat16)
        update = jnp.dot(node_hidden, w_node_out, preferred_element_type=jnp.float32)
        centred = update - lax.optimization_barrier(jnp.mean(update, axis=1, keepdims=True))
        variance = lax.optimization_barrier(jnp.mean(centred * centred, axis=1, keepdims=True))
        normed = centred * lax.rsqrt(variance + 1e-05)
        return (own.astype(jnp.float32) + normed * out_gain).astype(jnp.bfloat16)
    blocks = lax.map(one_block, jnp.arange(N_GX * N_GY * N_GZ, dtype=jnp.int32))
    return blocks.reshape(-1, width)
```

```python
import functools
import math

import jax
import jax.numpy as jnp
from jax import lax
from jax.experimental import pallas as pl
from jax.experimental.pallas import tpu as pltpu
from jax.sharding import PartitionSpec as P

BND = 512
AXES = ("gx", "gy", "gz")
F32 = jnp.float32
BF16 = jnp.bfloat16
TILE = 128


def mm(a, b):
    return jnp.dot(a, b, preferred_element_type=F32)


def silu(x):
    h = 0.5 * x
    return h + h * jnp.tanh(h)


def kernel(sizes, *refs):
    (node_h, clus_h, send_h, memb_h, wk_h, wv_h, wei_h, weo_h, wni_h, wno_h, gain_h) = refs[:11]
    out_ref = refs[11]
    (node, clus, send, memb, wk, wv, wei, weo, wni, wno, gain) = refs[12:23]
    rc = refs[23:26]
    rb = refs[26]
    kk, vv = refs[27], refs[28]
    table, rcv, gat, o_own, m_own, pooled = refs[29:35]
    loc_sem, cs_sem, cr_sem, bs_sem, br_sem = refs[35:40]

    count, width = node.shape
    ncl = clus.shape[0]
    deg = send.shape[0] * send.shape[1] // count
    c2 = math.log2(math.e) / math.sqrt(width)
    me = [lax.axis_index(a) for a in AXES]

    def at(axis, off):
        coords = list(me)
        coords[axis] = lax.rem(me[axis] + off, sizes[axis])
        return tuple(coords)

    barrier = pltpu.get_barrier_semaphore()
    greeted = 0
    for axis in range(3):
        for off in range(1, sizes[axis]):
            pl.semaphore_signal(
                barrier, inc=1, device_id=at(axis, off), device_id_type=pl.DeviceIdType.MESH
            )
            greeted += 1

    locals_ = []
    pairs = (
        (clus_h, clus), (wk_h, wk), (wv_h, wv), (node_h, node), (wei_h, wei), (memb_h, memb),
        (send_h, send), (wni_h, wni), (weo_h, weo), (wno_h, wno), (gain_h, gain),
    )
    for i, (src, dst) in enumerate(pairs):
        cp = pltpu.make_async_copy(src, dst, loc_sem.at[i])
        cp.start()
        locals_.append(cp)

    pl.semaphore_wait(barrier, greeted)

    clus_copies = [[], [], []]
    idx = 0
    for axis in (2, 1, 0):
        for off in range(1, sizes[axis]):
            cp = pltpu.make_async_remote_copy(
                src_ref=clus_h,
                dst_ref=rc[axis].at[pl.ds((off - 1) * ncl, ncl)],
                send_sem=cs_sem.at[idx],
                recv_sem=cr_sem.at[idx],
                device_id=at(axis, off),
                device_id_type=pl.DeviceIdType.MESH,
            )
            cp.start()
            clus_copies[axis].append(cp)
            idx += 1
    bnd_copies = {}
    for axis in (2, 1, 0):
        n = sizes[axis]
        for side, off in ((0, 1), (1, n - 1)):
            if side == 1 and n == 2:
                continue
            slot = 2 * axis + side
            cp = pltpu.make_async_remote_copy(
                src_ref=node_h.at[pl.ds(0, BND)],
                dst_ref=rb.at[slot],
                send_sem=bs_sem.at[slot],
                recv_sem=br_sem.at[slot],
                device_id=at(axis, off),
                device_id_type=pl.DeviceIdType.MESH,
            )
            cp.start()
            bnd_copies[slot] = cp

    for cp in locals_:
        cp.wait()

    ones = jnp.ones((ncl, width), BF16)

    def put_kv(rows, base):
        kk[pl.ds(base, ncl), :] = mm(rows, wk[...]).astype(BF16)
        vv[pl.ds(base, ncl), pl.ds(0, width)] = mm(rows, wv[...]).astype(BF16)
        vv[pl.ds(base, ncl), pl.ds(width, width)] = ones

    def attend(q, base, n):
        s = lax.dot_general(
            q, kk[pl.ds(base, n), :], (((1,), (1,)), ((), ())), preferred_element_type=F32
        )
        m = jnp.max(s, axis=1, keepdims=True)
        e = jnp.exp2((s - m) * c2).astype(BF16)
        return m, mm(e, vv[pl.ds(base, n), :])

    tiles = count // TILE

    put_kv(clus[...], 0)

    def first(t, carry):
        rows = pl.ds(pl.multiple_of(t * TILE, TILE), TILE)
        q = node[rows, :]
        table[rows, :] = mm(q, wei[pl.ds(width, width), :])
        rcv[rows, :] = mm(q, wei[pl.ds(0, width), :])
        m, o = attend(q, 0, ncl)
        m_own[rows, :] = jnp.broadcast_to(m, (TILE, width))
        o_own[rows, :] = o
        return carry

    lax.fori_loop(0, tiles, first, 0)

    base = ncl
    spans = []
    for axis in range(3):
        spans.append((base, (sizes[axis] - 1) * ncl))
        base += (sizes[axis] - 1) * ncl
    for axis in (2, 1, 0):
        for j, cp in enumerate(clus_copies[axis]):
            cp.wait_recv()
            put_kv(rc[axis][pl.ds(j * ncl, ncl), :], spans[axis][0] + j * ncl)

    def lines(t, carry):
        rows = pl.ds(pl.multiple_of(t * TILE, TILE), TILE)
        q = node[rows, :]
        m0 = m_own[rows, :]
        n0 = o_own[rows, pl.ds(0, width)]
        d0 = o_own[rows, pl.ds(width, width)]
        total = jnp.zeros((TILE, width), F32)
        for axis in range(3):
            m1, o1 = attend(q, *spans[axis])
            top = jnp.maximum(m0, m1)
            a0 = jnp.exp2((m0 - top) * c2)
            a1 = jnp.exp2((m1 - top) * c2)
            numer = a0 * n0 + a1 * o1[:, :width]
            denom = a0 * d0 + a1 * o1[:, width:]
            total = total + numer / denom
        att = total * lax.rsqrt(jnp.mean(total * total, axis=1, keepdims=True) + 1e-6)
        pooled[rows, :] = att.astype(BF16)
        return carry

    lax.fori_loop(0, tiles, lines, 0)

    for axis in (2, 1, 0):
        for side in range(2):
            slot = 2 * axis + side
            if slot not in bnd_copies:
                continue
            bnd_copies[slot].wait_recv()
            proj = mm(rb[slot], wei[pl.ds(width, width), :])
            table[pl.ds(count + slot * BND, BND), :] = proj
            if sizes[axis] == 2:
                table[pl.ds(count + (slot + 1) * BND, BND), :] = proj

    lane_rows = TILE * deg // send.shape[1]

    def gather(g, carry):
        for c in range(send.shape[1]):
            s = send[g, c]
            dst = g * (send.shape[1] // deg) + c // deg
            gat[c % deg, pl.ds(dst, 1), :] = table[pl.ds(s, 1), :]
        return carry

    lax.fori_loop(0, send.shape[0], gather, 0)

    cluster_ids = lax.broadcasted_iota(jnp.int32, (TILE, ncl), 1)

    def last(t, carry):
        rows = pl.ds(pl.multiple_of(t * TILE, TILE), TILE)
        q = node[rows, :]
        r = rcv[rows, :]
        hidden = silu(gat[0, rows, :] + r)
        for d in range(1, deg):
            hidden = hidden + silu(gat[d, rows, :] + r)
        agg = mm(hidden.astype(BF16), weo[...]).astype(BF16)
        ids = jnp.broadcast_to(memb[pl.ds(t, 1), :], (TILE, TILE)).T[:, :1]
        hot = jnp.where(cluster_ids == ids, 1.0, 0.0).astype(BF16)
        own = mm(hot, clus[...]).astype(BF16)
        pre = mm(jnp.concatenate([q, agg, pooled[rows, :], own], axis=1), wni[...])
        update = mm(silu(pre).astype(BF16), wno[...])
        cen = update - jnp.mean(update, axis=1, keepdims=True)
        var = jnp.mean(cen * cen, axis=1, keepdims=True)
        normed = cen * lax.rsqrt(var + 1e-5)
        out_ref[rows, :] = (q.astype(F32) + normed * gain[...]).astype(BF16)
        return carry

    lax.fori_loop(0, tiles, last, 0)

    for group in clus_copies:
        for cp in group:
            cp.wait_send()
    for cp in bnd_copies.values():
        cp.wait_send()


def solution(mesh):
    sizes = tuple(mesh.shape[a] for a in AXES)

    def on_device(node, clus, send, memb, wk, wv, wei, weo, wni, wno, gain):
        count, width = node.shape
        ncl = clus.shape[0]
        deg = send.size // count
        memb = memb.reshape(count // TILE, TILE)
        gain = gain.reshape(1, width)
        args = (node, clus, send, memb, wk, wv, wei, weo, wni, wno, gain)
        peers = sum(n - 1 for n in sizes)
        total = ncl * (1 + peers)
        scratch = []
        for i, a in enumerate(args):
            space = pltpu.SMEM if i == 2 else pltpu.VMEM
            scratch.append(space(a.shape, a.dtype))
        scratch += [pltpu.VMEM(((n - 1) * ncl, width), BF16) for n in sizes]
        scratch += [
            pltpu.VMEM((6, BND, width), BF16),
            pltpu.VMEM((total, width), BF16),
            pltpu.VMEM((total, 2 * width), BF16),
            pltpu.VMEM((count + 6 * BND, width), F32),
            pltpu.VMEM((count, width), F32),
            pltpu.VMEM((deg, count, width), F32),
            pltpu.VMEM((count, 2 * width), F32),
            pltpu.VMEM((count, width), F32),
            pltpu.VMEM((count, width), BF16),
            pltpu.SemaphoreType.DMA((len(args),)),
            pltpu.SemaphoreType.DMA((peers,)),
            pltpu.SemaphoreType.DMA((peers,)),
            pltpu.SemaphoreType.DMA((6,)),
            pltpu.SemaphoreType.DMA((6,)),
        ]
        return pl.pallas_call(
            functools.partial(kernel, sizes),
            out_shape=jax.ShapeDtypeStruct((count, width), BF16),
            in_specs=[pl.BlockSpec(memory_space=pl.ANY)] * len(args),
            out_specs=pl.BlockSpec(memory_space=pltpu.VMEM),
            scratch_shapes=scratch,
            compiler_params=pltpu.CompilerParams(
                collective_id=0, has_side_effects=True, vmem_limit_bytes=48 * 1024 * 1024
            ),
        )(*args)

    spec = P(AXES, None)
    return jax.shard_map(
        on_device,
        mesh=mesh,
        in_specs=(spec, spec, spec, P(AXES)) + (P(),) * 7,
        out_specs=spec,
        check_vma=False,
    )
```

```python
import functools
import math

import jax
import jax.numpy as jnp
from jax import lax
from jax.experimental import pallas as pl
from jax.experimental.pallas import tpu as pltpu
from jax.sharding import PartitionSpec as P

BND = 512
AXES = ("gx", "gy", "gz")
F32 = jnp.float32
BF16 = jnp.bfloat16
TILE = 128
TA = 256
TZ = 256


def mm(a, b):
    return jnp.dot(a, b, preferred_element_type=F32)


def silu(x):
    h = 0.5 * x
    return h + h * jnp.tanh(h)


def kernel(sizes, *refs):
    (node_h, clus_h, send_h, memb_h, wk_h, wv_h, wei_h, weo_h, wni_h, wno_h, gain_h) = refs[:11]
    out_ref = refs[11]
    (node, clus, send, memb, wk, wv, wei, weo, wni, wno, gain) = refs[12:23]
    rc = refs[23:26]
    rb = refs[26]
    kk, vv = refs[27], refs[28]
    table, rcv, gat, o_own, m_own, pooled, pre = refs[29:36]
    loc_sem, cs_sem, cr_sem, bs_sem, br_sem, zs_sem, zr_sem = refs[36:43]

    count, width = node.shape
    ncl = clus.shape[0]
    deg = send.shape[0] * send.shape[1] // count
    c2 = math.log2(math.e) / math.sqrt(width)
    me = [lax.axis_index(a) for a in AXES]

    def at(axis, off):
        coords = list(me)
        coords[axis] = lax.rem(me[axis] + off, sizes[axis])
        return tuple(coords)

    barrier = pltpu.get_barrier_semaphore()
    greeted = 0
    for axis in range(3):
        for off in range(1, sizes[axis]):
            pl.semaphore_signal(
                barrier, inc=1, device_id=at(axis, off), device_id_type=pl.DeviceIdType.MESH
            )
            greeted += 1

    locals_ = []
    pairs = (
        (clus_h, clus), (wk_h, wk), (wv_h, wv), (node_h, node), (wei_h, wei), (memb_h, memb),
        (send_h, send), (wni_h, wni), (weo_h, weo), (wno_h, wno), (gain_h, gain),
    )
    for i, (src, dst) in enumerate(pairs):
        cp = pltpu.make_async_copy(src, dst, loc_sem.at[i])
        cp.start()
        locals_.append(cp)

    with jax.named_scope("p_barrier"):
        pl.semaphore_wait(barrier, greeted)

    zn = sizes[2]
    zi = me[2]

    def remote(src, dst, ssem, rsem, dev):
        return pltpu.make_async_remote_copy(
            src_ref=src, dst_ref=dst, send_sem=ssem, recv_sem=rsem,
            device_id=dev, device_id_type=pl.DeviceIdType.MESH,
        )

    def z_slot(i):
        return rc[2].at[pl.ds(i * ncl, ncl)]

    def hop(step, up):
        i = step if up else zn - 2 - step
        j = step - 1 if up else zn - 1 - step
        src = clus_h if step == 0 else z_slot(j)
        k = 2 * step + (0 if up else 1)
        go = jnp.logical_and(zi >= step, zi < zn - 1) if up else jnp.logical_and(zi < zn - step, zi > 0)
        return go, remote(src, z_slot(i), zs_sem.at[k], zr_sem.at[i], at(2, 1 if up else zn - 1))

    def z_recv(i):
        return remote(clus_h, z_slot(i), zs_sem.at[0], zr_sem.at[i], at(2, 1))

    def start_hop(step):
        for up in (True, False):
            go, cp = hop(step, up)

            @pl.when(go)
            def _():
                if step > 0:
                    z_recv(step - 1 if up else zn - 1 - step).wait_recv()
                cp.start()

    def boundary(axis):
        n = sizes[axis]
        for side, off in ((0, 1), (1, n - 1)):
            if side == 1 and n == 2:
                continue
            slot = 2 * axis + side
            cp = remote(node_h.at[pl.ds(0, BND)], rb.at[slot], bs_sem.at[slot], br_sem.at[slot], at(axis, off))
            cp.start()
            bnd_copies[slot] = cp

    bnd_copies = {}
    clus_copies = [[], []]
    start_hop(0)
    boundary(2)
    idx = 0
    for axis in (0, 1):
        for off in range(1, sizes[axis]):
            cp = remote(
                clus_h, rc[axis].at[pl.ds((off - 1) * ncl, ncl)], cs_sem.at[idx], cr_sem.at[idx], at(axis, off)
            )
            cp.start()
            clus_copies[axis].append(cp)
            idx += 1
    boundary(0)
    boundary(1)

    with jax.named_scope("p_local"):
        for cp in locals_:
            cp.wait()

    ones = jnp.ones((ncl, width), BF16)

    def put_kv(rows, base):
        kk[pl.ds(base, ncl), :] = mm(rows, wk[...]).astype(BF16)
        vv[pl.ds(base, ncl), pl.ds(0, width)] = mm(rows, wv[...]).astype(BF16)
        vv[pl.ds(base, ncl), pl.ds(width, width)] = ones

    def attend(q, base, n):
        s = lax.dot_general(
            q, kk[pl.ds(base, n), :], (((1,), (1,)), ((), ())), preferred_element_type=F32
        )
        m = jnp.max(s, axis=1, keepdims=True)
        e = jnp.exp2((s - m) * c2).astype(BF16)
        return m, mm(e, vv[pl.ds(base, n), :])

    put_kv(clus[...], 0)
    cluster_ids = lax.broadcasted_iota(jnp.int32, (TILE, ncl), 1)

    def first(t, carry):
        rows = pl.ds(pl.multiple_of(t * TA, TA), TA)
        q = node[rows, :]
        table[rows, :] = mm(q, wei[pl.ds(width, width), :])
        rcv[rows, :] = mm(q, wei[pl.ds(0, width), :])
        hots = []
        for j in range(TA // TILE):
            ids = jnp.broadcast_to(memb[pl.ds(t * (TA // TILE) + j, 1), :], (TILE, TILE)).T[:, :1]
            hots.append(jnp.where(cluster_ids == ids, 1.0, 0.0).astype(BF16))
        own = mm(jnp.concatenate(hots, axis=0), clus[...]).astype(BF16)
        pre[rows, :] = mm(q, wni[pl.ds(0, width), :]) + mm(own, wni[pl.ds(3 * width, width), :])
        m, o = attend(q, 0, ncl)
        m_own[rows, :] = jnp.broadcast_to(m, (TA, width))
        o_own[rows, :] = o
        return carry

    with jax.named_scope("p_first"):
        lax.fori_loop(0, count // TA, first, 0)

    for step in range(1, min(2, zn - 1)):
        with jax.named_scope("p_hop1"):
            start_hop(step)

    base = ncl
    spans = []
    for axis in range(3):
        spans.append((base, (sizes[axis] - 1) * ncl))
        base += (sizes[axis] - 1) * ncl
    for axis in (0, 1):
        for j, cp in enumerate(clus_copies[axis]):
            with jax.named_scope("p_wkv"):
                cp.wait_recv()
            put_kv(rc[axis][pl.ds(j * ncl, ncl), :], spans[axis][0] + j * ncl)

    def line(q, rows, axis):
        m0 = m_own[rows, :]
        n0 = o_own[rows, pl.ds(0, width)]
        d0 = o_own[rows, pl.ds(width, width)]
        m1, o1 = attend(q, *spans[axis])
        top = jnp.maximum(m0, m1)
        a0 = jnp.exp2((m0 - top) * c2)
        a1 = jnp.exp2((m1 - top) * c2)
        numer = a0 * n0 + a1 * o1[:, :width]
        denom = a0 * d0 + a1 * o1[:, width:]
        return numer / denom

    def lines(t, carry):
        rows = pl.ds(pl.multiple_of(t * TA, TA), TA)
        q = node[rows, :]
        pooled[rows, :] = line(q, rows, 0) + line(q, rows, 1)
        return carry

    with jax.named_scope("p_lines"):
        lax.fori_loop(0, count // TA, lines, 0)

    for step in range(2, zn - 1):
        with jax.named_scope("p_hop2"):
            start_hop(step)

    for axis in (0, 1, 2):
        for side in range(2):
            slot = 2 * axis + side
            if slot not in bnd_copies:
                continue
            with jax.named_scope("p_wb"):
                bnd_copies[slot].wait_recv()
            proj = mm(rb[slot], wei[pl.ds(width, width), :])
            table[pl.ds(count + slot * BND, BND), :] = proj
            if sizes[axis] == 2:
                table[pl.ds(count + (slot + 1) * BND, BND), :] = proj

    lanes = send.shape[1]
    per = TILE * deg // lanes

    def gather(t):
        for g in range(per):
            for c in range(lanes):
                s = send[t * per + g, c]
                dst = t * TILE + (g * lanes + c) // deg
                gat[c % deg, pl.ds(dst, 1), :] = table[pl.ds(s, 1), :]

    def edges(t):
        rows = pl.ds(pl.multiple_of(t * TILE, TILE), TILE)
        r = rcv[rows, :]
        hidden = silu(gat[0, rows, :] + r)
        for d in range(1, deg):
            hidden = hidden + silu(gat[d, rows, :] + r)
        agg = mm(hidden.astype(BF16), weo[...]).astype(BF16)
        pre[rows, :] = pre[rows, :] + mm(agg, wni[pl.ds(width, width), :])

    def edge_step(t, carry):
        edges(t - 1)
        gather(t)
        return carry

    with jax.named_scope("p_gather"):
        gather(0)
        lax.fori_loop(1, count // TILE, edge_step, 0)
        edges(count // TILE - 1)

    for j in range(zn - 1):
        with jax.named_scope("p_wz"):
            passed = jnp.logical_or(
                jnp.logical_and(j < zi, jnp.logical_and(zi < zn - 1, j < zn - 2)),
                jnp.logical_and(j >= zi, jnp.logical_and(zi > 0, j > 0)),
            )

            @pl.when(jnp.logical_not(passed))
            def _():
                z_recv(j).wait_recv()
        put_kv(rc[2][pl.ds(j * ncl, ncl), :], spans[2][0] + j * ncl)

    def last(t, carry):
        rows = pl.ds(pl.multiple_of(t * TZ, TZ), TZ)
        q = node[rows, :]
        total = pooled[rows, :] + line(q, rows, 2)
        att = total * lax.rsqrt(jnp.mean(total * total, axis=1, keepdims=True) + 1e-6)
        p = pre[rows, :] + mm(att.astype(BF16), wni[pl.ds(2 * width, width), :])
        update = mm(silu(p).astype(BF16), wno[...])
        cen = update - jnp.mean(update, axis=1, keepdims=True)
        var = jnp.mean(cen * cen, axis=1, keepdims=True)
        normed = cen * lax.rsqrt(var + 1e-5)
        out_ref[rows, :] = (q.astype(F32) + normed * gain[...]).astype(BF16)
        return carry

    with jax.named_scope("p_last"):
        lax.fori_loop(0, count // TZ, last, 0)

    for group in clus_copies:
        for cp in group:
            cp.wait_send()
    for cp in bnd_copies.values():
        cp.wait_send()
    for step in range(zn - 1):
        for up in (True, False):
            go, cp = hop(step, up)

            @pl.when(go)
            def _():
                cp.wait_send()


def solution(mesh):
    sizes = tuple(mesh.shape[a] for a in AXES)

    def on_device(node, clus, send, memb, wk, wv, wei, weo, wni, wno, gain):
        count, width = node.shape
        ncl = clus.shape[0]
        deg = send.size // count
        memb = memb.reshape(count // TILE, TILE)
        gain = gain.reshape(1, width)
        args = (node, clus, send, memb, wk, wv, wei, weo, wni, wno, gain)
        peers = sum(n - 1 for n in sizes)
        total = ncl * (1 + peers)
        scratch = []
        for i, a in enumerate(args):
            space = pltpu.SMEM if i == 2 else pltpu.VMEM
            scratch.append(space(a.shape, a.dtype))
        scratch += [pltpu.VMEM(((n - 1) * ncl, width), BF16) for n in sizes]
        scratch += [
            pltpu.VMEM((6, BND, width), BF16),
            pltpu.VMEM((total, width), BF16),
            pltpu.VMEM((total, 2 * width), BF16),
            pltpu.VMEM((count + 6 * BND, width), F32),
            pltpu.VMEM((count, width), F32),
            pltpu.VMEM((deg, count, width), F32),
            pltpu.VMEM((count, 2 * width), F32),
            pltpu.VMEM((count, width), F32),
            pltpu.VMEM((count, width), F32),
            pltpu.VMEM((count, width), F32),
            pltpu.SemaphoreType.DMA((len(args),)),
            pltpu.SemaphoreType.DMA((peers,)),
            pltpu.SemaphoreType.DMA((peers,)),
            pltpu.SemaphoreType.DMA((6,)),
            pltpu.SemaphoreType.DMA((6,)),
            pltpu.SemaphoreType.DMA((2 * sizes[2],)),
            pltpu.SemaphoreType.DMA((sizes[2],)),
        ]
        return pl.pallas_call(
            functools.partial(kernel, sizes),
            out_shape=jax.ShapeDtypeStruct((count, width), BF16),
            in_specs=[pl.BlockSpec(memory_space=pltpu.HBM)] * len(args),
            out_specs=pl.BlockSpec(memory_space=pltpu.VMEM),
            scratch_shapes=scratch,
            compiler_params=pltpu.CompilerParams(
                collective_id=0, has_side_effects=True
            ),
        )(*args)

    spec = P(AXES, None)
    return jax.shard_map(
        on_device,
        mesh=mesh,
        in_specs=(spec, spec, spec, P(AXES)) + (P(),) * 7,
        out_specs=spec,
        check_vma=False,
    )
```

```python
import functools
import math

import jax
import jax.numpy as jnp
from jax import lax
from jax.experimental import pallas as pl
from jax.experimental.pallas import tpu as pltpu
from jax.sharding import PartitionSpec as P

BND = 512
AXES = ("gx", "gy", "gz")
F32 = jnp.float32
BF16 = jnp.bfloat16
TILE = 128
TA = 512
TZ = 512


def mm(a, b):
    return jnp.dot(a, b, preferred_element_type=F32)


def silu(x):
    h = 0.5 * x
    return h + h * jnp.tanh(h)


def kernel(sizes, *refs):
    (node_h, clus_h, send_h, memb_h, wk_h, wv_h, wei_h, weo_h, wni_h, wno_h, gain_h) = refs[:11]
    out_ref = refs[11]
    (node, clus, send, memb, wk, wv, wei, weo, wni, wno, gain) = refs[12:23]
    rc = refs[23:26]
    rb = refs[26]
    kk, vv = refs[27], refs[28]
    table, rcv, gat, o_own, m_own, pooled, pre = refs[29:36]
    loc_sem, cs_sem, cr_sem, bs_sem, br_sem, zs_sem, zr_sem = refs[36:43]

    count, width = node.shape
    ncl = clus.shape[0]
    deg = send.shape[0] * send.shape[1] // count
    c2 = math.log2(math.e) / math.sqrt(width)
    me = [lax.axis_index(a) for a in AXES]

    def at(axis, off):
        coords = list(me)
        coords[axis] = lax.rem(me[axis] + off, sizes[axis])
        return tuple(coords)

    barrier = pltpu.get_barrier_semaphore()
    greeted = 0
    for axis in range(3):
        for off in range(1, sizes[axis]):
            pl.semaphore_signal(
                barrier, inc=1, device_id=at(axis, off), device_id_type=pl.DeviceIdType.MESH
            )
            greeted += 1

    locals_ = []
    pairs = (
        (clus_h, clus), (wk_h, wk), (wv_h, wv), (node_h, node), (wei_h, wei), (memb_h, memb),
        (send_h, send), (wni_h, wni), (weo_h, weo), (wno_h, wno), (gain_h, gain),
    )
    for i, (src, dst) in enumerate(pairs):
        cp = pltpu.make_async_copy(src, dst, loc_sem.at[i])
        cp.start()
        locals_.append(cp)

    vv[:, pl.ds(width, width)] = jnp.ones((vv.shape[0], width), BF16)

    with jax.named_scope("p_barrier"):
        pl.semaphore_wait(barrier, greeted)

    zn = sizes[2]
    zi = me[2]

    def remote(src, dst, ssem, rsem, dev):
        return pltpu.make_async_remote_copy(
            src_ref=src, dst_ref=dst, send_sem=ssem, recv_sem=rsem,
            device_id=dev, device_id_type=pl.DeviceIdType.MESH,
        )

    def z_slot(i):
        return rc[2].at[pl.ds(i * ncl, ncl)]

    def hop(step, up):
        i = step if up else zn - 2 - step
        j = step - 1 if up else zn - 1 - step
        src = clus_h if step == 0 else z_slot(j)
        k = 2 * step + (0 if up else 1)
        go = jnp.logical_and(zi >= step, zi < zn - 1) if up else jnp.logical_and(zi < zn - step, zi > 0)
        return go, remote(src, z_slot(i), zs_sem.at[k], zr_sem.at[i], at(2, 1 if up else zn - 1))

    def z_recv(i):
        return remote(clus_h, z_slot(i), zs_sem.at[0], zr_sem.at[i], at(2, 1))

    def start_hop(step):
        for up in (True, False):
            go, cp = hop(step, up)

            @pl.when(go)
            def _():
                if step > 0:
                    z_recv(step - 1 if up else zn - 1 - step).wait_recv()
                cp.start()

    def boundary(axis):
        n = sizes[axis]
        for side, off in ((0, 1), (1, n - 1)):
            if side == 1 and n == 2:
                continue
            slot = 2 * axis + side
            cp = remote(node_h.at[pl.ds(0, BND)], rb.at[slot], bs_sem.at[slot], br_sem.at[slot], at(axis, off))
            cp.start()
            bnd_copies[slot] = cp

    bnd_copies = {}
    clus_copies = [[], []]
    start_hop(0)
    boundary(2)
    idx = 0
    for axis in (0, 1):
        for off in range(1, sizes[axis]):
            cp = remote(
                clus_h, rc[axis].at[pl.ds((off - 1) * ncl, ncl)], cs_sem.at[idx], cr_sem.at[idx], at(axis, off)
            )
            cp.start()
            clus_copies[axis].append(cp)
            idx += 1
    boundary(0)
    boundary(1)

    with jax.named_scope("p_local"):
        for cp in locals_:
            cp.wait()

    def put_kv(rows, base):
        n = rows.shape[0]
        kk[:, pl.ds(base, n)] = mm(rows, wk[...]).T.astype(BF16)
        vv[pl.ds(base, n), pl.ds(0, width)] = mm(rows, wv[...]).astype(BF16)

    def score(q, base, n):
        return mm(q, kk[:, pl.ds(base, n)])

    def weigh(s, base, n):
        m = jnp.max(s, axis=1, keepdims=True)
        e = jnp.exp2((s - m) * c2).astype(BF16)
        return m, mm(e, vv[pl.ds(base, n), :])

    put_kv(clus[...], 0)
    cluster_ids = lax.broadcasted_iota(jnp.int32, (TILE, ncl), 1)

    def first(t):
        rows = pl.ds(t * TA, TA)
        q = node[rows, :]
        table[rows, :] = mm(q, wei[pl.ds(width, width), :])
        rcv[rows, :] = mm(q, wei[pl.ds(0, width), :])
        hots = []
        for j in range(TA // TILE):
            ids = jnp.broadcast_to(memb[pl.ds(t * (TA // TILE) + j, 1), :], (TILE, TILE)).T[:, :1]
            hots.append(jnp.where(cluster_ids == ids, 1.0, 0.0).astype(BF16))
        own = mm(jnp.concatenate(hots, axis=0), clus[...]).astype(BF16)
        pre[rows, :] = mm(q, wni[pl.ds(0, width), :]) + mm(own, wni[pl.ds(3 * width, width), :])
        m, o = weigh(score(q, 0, ncl), 0, ncl)
        m_own[rows, :] = jnp.broadcast_to(m, (TA, width))
        o_own[rows, :] = o

    with jax.named_scope("p_first"):
        for t in range(count // TA):
            first(t)

    for step in range(1, min(2, zn - 1)):
        with jax.named_scope("p_hop1"):
            start_hop(step)

    base = ncl
    spans = []
    for axis in range(3):
        spans.append((base, (sizes[axis] - 1) * ncl))
        base += (sizes[axis] - 1) * ncl
    with jax.named_scope("p_wkv"):
        for axis in (0, 1):
            for cp in clus_copies[axis]:
                cp.wait_recv()
    for axis in (0, 1):
        put_kv(rc[axis][...], spans[axis][0])

    def line(s, rows, axis):
        m0 = m_own[rows, :]
        n0 = o_own[rows, pl.ds(0, width)]
        d0 = o_own[rows, pl.ds(width, width)]
        m1, o1 = weigh(s, *spans[axis])
        top = jnp.maximum(m0, m1)
        a0 = jnp.exp2((m0 - top) * c2)
        a1 = jnp.exp2((m1 - top) * c2)
        numer = a0 * n0 + a1 * o1[:, :width]
        denom = a0 * d0 + a1 * o1[:, width:]
        return numer / denom

    def pipeline(size, ready, use):
        spots = [pl.ds(i, size) for i in range(0, count, size)]
        ahead = ready(spots[0])
        for i, rows in enumerate(spots):
            now = ahead
            if i + 1 < len(spots):
                ahead = ready(spots[i + 1])
            use(rows, now)

    def lines_ready(rows):
        q = node[rows, :]
        return score(q, *spans[0]), score(q, *spans[1])

    def lines_use(rows, now):
        pooled[rows, :] = line(now[0], rows, 0) + line(now[1], rows, 1)

    with jax.named_scope("p_lines"):
        pipeline(TA, lines_ready, lines_use)

    for step in range(2, zn - 1):
        with jax.named_scope("p_hop2"):
            start_hop(step)

    with jax.named_scope("p_wb"):
        for cp in bnd_copies.values():
            cp.wait_recv()
    for slot in bnd_copies:
        proj = mm(rb[slot], wei[pl.ds(width, width), :])
        table[pl.ds(count + slot * BND, BND), :] = proj
        if sizes[slot // 2] == 2:
            table[pl.ds(count + (slot + 1) * BND, BND), :] = proj

    lanes = send.shape[1]
    per = TILE * deg // lanes

    def gather(t):
        for g in range(per):
            for c in range(lanes):
                s = send[t * per + g, c]
                dst = t * TILE + (g * lanes + c) // deg
                gat[c % deg, pl.ds(dst, 1), :] = table[pl.ds(s, 1), :]

    def edges(t):
        rows = pl.ds(t * TILE, TILE)
        r = rcv[rows, :]
        hidden = silu(gat[0, rows, :] + r)
        for d in range(1, deg):
            hidden = hidden + silu(gat[d, rows, :] + r)
        agg = mm(hidden.astype(BF16), weo[...]).astype(BF16)
        pre[rows, :] = pre[rows, :] + mm(agg, wni[pl.ds(width, width), :])

    with jax.named_scope("p_gather"):
        gather(0)
        for t in range(1, count // TILE):
            edges(t - 1)
            gather(t)
        edges(count // TILE - 1)

    for j in range(zn - 1):
        with jax.named_scope("p_wz"):
            passed = jnp.logical_or(
                jnp.logical_and(j < zi, jnp.logical_and(zi < zn - 1, j < zn - 2)),
                jnp.logical_and(j >= zi, jnp.logical_and(zi > 0, j > 0)),
            )

            @pl.when(jnp.logical_not(passed))
            def _():
                z_recv(j).wait_recv()

    put_kv(rc[2][...], spans[2][0])

    def last_ready(rows):
        return score(node[rows, :], *spans[2])

    def last_use(rows, now):
        total = pooled[rows, :] + line(now, rows, 2)
        att = total * lax.rsqrt(jnp.mean(total * total, axis=1, keepdims=True) + 1e-6)
        p = pre[rows, :] + mm(att.astype(BF16), wni[pl.ds(2 * width, width), :])
        update = mm(silu(p).astype(BF16), wno[...])
        cen = update - jnp.mean(update, axis=1, keepdims=True)
        var = jnp.mean(cen * cen, axis=1, keepdims=True)
        normed = cen * lax.rsqrt(var + 1e-5)
        out_ref[rows, :] = (node[rows, :].astype(F32) + normed * gain[...]).astype(BF16)

    with jax.named_scope("p_last"):
        pipeline(TZ, last_ready, last_use)

    for group in clus_copies:
        for cp in group:
            cp.wait_send()
    for cp in bnd_copies.values():
        cp.wait_send()
    for step in range(zn - 1):
        for up in (True, False):
            go, cp = hop(step, up)

            @pl.when(go)
            def _():
                cp.wait_send()


def solution(mesh):
    sizes = tuple(mesh.shape[a] for a in AXES)

    def on_device(node, clus, send, memb, wk, wv, wei, weo, wni, wno, gain):
        count, width = node.shape
        ncl = clus.shape[0]
        deg = send.size // count
        memb = memb.reshape(count // TILE, TILE)
        gain = gain.reshape(1, width)
        args = (node, clus, send, memb, wk, wv, wei, weo, wni, wno, gain)
        peers = sum(n - 1 for n in sizes)
        total = ncl * (1 + peers)
        scratch = []
        for i, a in enumerate(args):
            space = pltpu.SMEM if i == 2 else pltpu.VMEM
            scratch.append(space(a.shape, a.dtype))
        scratch += [pltpu.VMEM(((n - 1) * ncl, width), BF16) for n in sizes]
        scratch += [
            pltpu.VMEM((6, BND, width), BF16),
            pltpu.VMEM((width, total), BF16),
            pltpu.VMEM((total, 2 * width), BF16),
            pltpu.VMEM((count + 6 * BND, width), F32),
            pltpu.VMEM((count, width), F32),
            pltpu.VMEM((deg, count, width), F32),
            pltpu.VMEM((count, 2 * width), F32),
            pltpu.VMEM((count, width), F32),
            pltpu.VMEM((count, width), F32),
            pltpu.VMEM((count, width), F32),
            pltpu.SemaphoreType.DMA((len(args),)),
            pltpu.SemaphoreType.DMA((peers,)),
            pltpu.SemaphoreType.DMA((peers,)),
            pltpu.SemaphoreType.DMA((6,)),
            pltpu.SemaphoreType.DMA((6,)),
            pltpu.SemaphoreType.DMA((2 * sizes[2],)),
            pltpu.SemaphoreType.DMA((sizes[2],)),
        ]
        return pl.pallas_call(
            functools.partial(kernel, sizes),
            out_shape=jax.ShapeDtypeStruct((count, width), BF16),
            in_specs=[pl.BlockSpec(memory_space=pltpu.HBM)] * len(args),
            out_specs=pl.BlockSpec(memory_space=pltpu.VMEM),
            scratch_shapes=scratch,
            compiler_params=pltpu.CompilerParams(
                collective_id=0, has_side_effects=True
            ),
        )(*args)

    spec = P(AXES, None)
    return jax.shard_map(
        on_device,
        mesh=mesh,
        in_specs=(spec, spec, spec, P(AXES)) + (P(),) * 7,
        out_specs=spec,
        check_vma=False,
    )
```

```python
import functools
import math

import jax
import jax.numpy as jnp
from jax import lax
from jax.experimental import pallas as pl
from jax.experimental.pallas import tpu as pltpu
from jax.sharding import PartitionSpec as P

BND = 512
AXES = ("gx", "gy", "gz")
F32 = jnp.float32
BF16 = jnp.bfloat16
TILE = 128
TA = 512
TZ = 512


def mm(a, b):
    return jnp.dot(a, b, preferred_element_type=F32)


def silu(x):
    h = 0.5 * x
    return h + h * jnp.tanh(h)


def kernel(sizes, *refs):
    (node_h, clus_h, send_h, memb_h, wk_h, wv_h, wei_h, weo_h, wni_h, wno_h, gain_h) = refs[:11]
    out_ref = refs[11]
    (node, clus, send, memb, wk, wv, wei, weo, wni, wno, gain) = refs[12:23]
    rc = refs[23:26]
    rb = refs[26]
    kk, vv = refs[27], refs[28]
    table, rcv, gat, o_own, m_own, pooled, pre = refs[29:36]
    loc_sem, cs_sem, cr_sem, bs_sem, br_sem, zs_sem, zr_sem = refs[36:43]

    count, width = node.shape
    ncl = clus.shape[0]
    deg = send.shape[0] * send.shape[1] // count
    c2 = math.log2(math.e) / math.sqrt(width)
    me = [lax.axis_index(a) for a in AXES]

    def at(axis, off):
        coords = list(me)
        coords[axis] = lax.rem(me[axis] + off, sizes[axis])
        return tuple(coords)

    barrier = pltpu.get_barrier_semaphore()
    greeted = 0
    for axis in range(3):
        near = sorted({1, sizes[2] - 1} | set(range(3, sizes[2])) | set(range(1, sizes[2] - 2)))
        for off in range(1, sizes[axis]) if axis < 2 else near:
            pl.semaphore_signal(
                barrier, inc=1, device_id=at(axis, off), device_id_type=pl.DeviceIdType.MESH
            )
            greeted += 1

    locals_ = []
    pairs = (
        (clus_h, clus), (wk_h, wk), (wv_h, wv), (node_h, node), (wei_h, wei), (memb_h, memb),
        (send_h, send), (wni_h, wni), (weo_h, weo), (wno_h, wno), (gain_h, gain),
    )
    for i, (src, dst) in enumerate(pairs):
        cp = pltpu.make_async_copy(src, dst, loc_sem.at[i])
        cp.start()
        locals_.append(cp)

    vv[:, pl.ds(width, width)] = jnp.ones((vv.shape[0], width), BF16)

    with jax.named_scope("p_barrier"):
        pl.semaphore_wait(barrier, greeted)

    zn = sizes[2]
    zi = me[2]

    def remote(src, dst, ssem, rsem, dev):
        return pltpu.make_async_remote_copy(
            src_ref=src, dst_ref=dst, send_sem=ssem, recv_sem=rsem,
            device_id=dev, device_id_type=pl.DeviceIdType.MESH,
        )

    def z_slot(i):
        return rc[2].at[pl.ds(i * ncl, ncl)]

    def hop(step, up):
        i = step if up else zn - 2 - step
        far = 1 if step < 2 else step + 1
        src = z_slot(0 if up else zn - 2) if step == 1 else clus_h
        k = 2 * step + (0 if up else 1)
        if step == 1:
            go = jnp.logical_and(zi > 0, zi < zn - 1)
        else:
            go = zi + far < zn if up else zi >= far
        return go, remote(src, z_slot(i), zs_sem.at[k], zr_sem.at[i], at(2, far if up else zn - far))

    def z_recv(i):
        return remote(clus_h, z_slot(i), zs_sem.at[0], zr_sem.at[i], at(2, 1))

    def start_hop(step):
        for up in (True, False):
            go, cp = hop(step, up)

            @pl.when(go)
            def _():
                if step == 1:
                    z_recv(0 if up else zn - 2).wait_recv()
                cp.start()

    def boundary(axis):
        n = sizes[axis]
        for side, off in ((0, 1), (1, n - 1)):
            if side == 1 and n == 2:
                continue
            slot = 2 * axis + side
            cp = remote(node_h.at[pl.ds(0, BND)], rb.at[slot], bs_sem.at[slot], br_sem.at[slot], at(axis, off))
            cp.start()
            bnd_copies[slot] = cp

    bnd_copies = {}
    clus_copies = [[], []]
    start_hop(0)
    for step in range(2, zn - 1):
        start_hop(step)
    boundary(2)
    idx = 0
    for axis in (0, 1):
        for off in range(1, sizes[axis]):
            cp = remote(
                clus_h, rc[axis].at[pl.ds((off - 1) * ncl, ncl)], cs_sem.at[idx], cr_sem.at[idx], at(axis, off)
            )
            cp.start()
            clus_copies[axis].append(cp)
            idx += 1
    boundary(0)
    boundary(1)

    with jax.named_scope("p_local"):
        for cp in locals_:
            cp.wait()

    def put_kv(rows, base):
        n = rows.shape[0]
        kk[:, pl.ds(base, n)] = mm(rows, wk[...]).T.astype(BF16)
        vv[pl.ds(base, n), pl.ds(0, width)] = mm(rows, wv[...]).astype(BF16)

    def score(q, base, n):
        return mm(q, kk[:, pl.ds(base, n)])

    def weigh(s, base, n):
        m = jnp.max(s, axis=1, keepdims=True)
        e = jnp.exp2((s - m) * c2).astype(BF16)
        return m, mm(e, vv[pl.ds(base, n), :])

    put_kv(clus[...], 0)
    cluster_ids = lax.broadcasted_iota(jnp.int32, (TILE, ncl), 1)

    def first(t):
        rows = pl.ds(t * TA, TA)
        q = node[rows, :]
        table[rows, :] = mm(q, wei[pl.ds(width, width), :])
        rcv[rows, :] = mm(q, wei[pl.ds(0, width), :])
        hots = []
        for j in range(TA // TILE):
            ids = jnp.broadcast_to(memb[pl.ds(t * (TA // TILE) + j, 1), :], (TILE, TILE)).T[:, :1]
            hots.append(jnp.where(cluster_ids == ids, 1.0, 0.0).astype(BF16))
        own = mm(jnp.concatenate(hots, axis=0), clus[...]).astype(BF16)
        pre[rows, :] = mm(q, wni[pl.ds(0, width), :]) + mm(own, wni[pl.ds(3 * width, width), :])
        m, o = weigh(score(q, 0, ncl), 0, ncl)
        m_own[rows, :] = jnp.broadcast_to(m, (TA, width))
        o_own[rows, :] = o

    with jax.named_scope("p_first"):
        for t in range(count // TA):
            first(t)

    for step in range(1, min(2, zn - 1)):
        with jax.named_scope("p_hop1"):
            start_hop(step)

    base = ncl
    spans = []
    for axis in range(3):
        spans.append((base, (sizes[axis] - 1) * ncl))
        base += (sizes[axis] - 1) * ncl
    with jax.named_scope("p_wkv"):
        for axis in (0, 1):
            for cp in clus_copies[axis]:
                cp.wait_recv()
    for axis in (0, 1):
        put_kv(rc[axis][...], spans[axis][0])

    def line(s, rows, axis):
        m0 = m_own[rows, :]
        n0 = o_own[rows, pl.ds(0, width)]
        d0 = o_own[rows, pl.ds(width, width)]
        m1, o1 = weigh(s, *spans[axis])
        top = jnp.maximum(m0, m1)
        a0 = jnp.exp2((m0 - top) * c2)
        a1 = jnp.exp2((m1 - top) * c2)
        numer = a0 * n0 + a1 * o1[:, :width]
        denom = a0 * d0 + a1 * o1[:, width:]
        return numer / denom

    def pipeline(size, ready, use):
        spots = [pl.ds(i, size) for i in range(0, count, size)]
        ahead = ready(spots[0])
        for i, rows in enumerate(spots):
            now = ahead
            if i + 1 < len(spots):
                ahead = ready(spots[i + 1])
            use(rows, now)

    def lines_ready(rows):
        q = node[rows, :]
        return score(q, *spans[0]), score(q, *spans[1])

    def lines_use(rows, now):
        pooled[rows, :] = line(now[0], rows, 0) + line(now[1], rows, 1)

    with jax.named_scope("p_lines"):
        pipeline(TA, lines_ready, lines_use)

    for j in range(zn - 1):
        with jax.named_scope("p_wz"):
            passed = jnp.logical_and(zi > 0, zi < zn - 1) if j in (0, zn - 2) and zn > 2 else zi < 0

            @pl.when(jnp.logical_not(passed))
            def _():
                z_recv(j).wait_recv()

    put_kv(rc[2][...], spans[2][0])

    def last_ready(rows):
        return score(node[rows, :], *spans[2])

    def last_use(rows, now):
        total = pooled[rows, :] + line(now, rows, 2)
        att = total * lax.rsqrt(jnp.mean(total * total, axis=1, keepdims=True) + 1e-6)
        pre[rows, :] = pre[rows, :] + mm(att.astype(BF16), wni[pl.ds(2 * width, width), :])

    with jax.named_scope("p_zline"):
        pipeline(TZ, last_ready, last_use)

    with jax.named_scope("p_wb"):
        for cp in bnd_copies.values():
            cp.wait_recv()
    for slot in bnd_copies:
        proj = mm(rb[slot], wei[pl.ds(width, width), :])
        table[pl.ds(count + slot * BND, BND), :] = proj
        if sizes[slot // 2] == 2:
            table[pl.ds(count + (slot + 1) * BND, BND), :] = proj

    lanes = send.shape[1]
    per = TILE * deg // lanes

    def gather(t):
        for g in range(per):
            for c in range(lanes):
                s = send[t * per + g, c]
                dst = t * TILE + (g * lanes + c) // deg
                gat[c % deg, pl.ds(dst, 1), :] = table[pl.ds(s, 1), :]

    def edges(t):
        rows = pl.ds(t * TILE, TILE)
        r = rcv[rows, :]
        hidden = silu(gat[0, rows, :] + r)
        for d in range(1, deg):
            hidden = hidden + silu(gat[d, rows, :] + r)
        agg = mm(hidden.astype(BF16), weo[...]).astype(BF16)
        pre[rows, :] = pre[rows, :] + mm(agg, wni[pl.ds(width, width), :])

    def nodes(t):
        rows = pl.ds(t * TILE, TILE)
        update = mm(silu(pre[rows, :]).astype(BF16), wno[...])
        cen = update - jnp.mean(update, axis=1, keepdims=True)
        var = jnp.mean(cen * cen, axis=1, keepdims=True)
        normed = cen * lax.rsqrt(var + 1e-5)
        out_ref[rows, :] = (node[rows, :].astype(F32) + normed * gain[...]).astype(BF16)

    with jax.named_scope("p_gather"):
        tiles = count // TILE
        for t in range(tiles + 2):
            if t >= 2:
                nodes(t - 2)
            if 1 <= t <= tiles:
                edges(t - 1)
            if t < tiles:
                gather(t)

    for group in clus_copies:
        for cp in group:
            cp.wait_send()
    for cp in bnd_copies.values():
        cp.wait_send()
    for step in range(zn - 1):
        for up in (True, False):
            go, cp = hop(step, up)

            @pl.when(go)
            def _():
                cp.wait_send()


def solution(mesh):
    sizes = tuple(mesh.shape[a] for a in AXES)

    def on_device(node, clus, send, memb, wk, wv, wei, weo, wni, wno, gain):
        count, width = node.shape
        ncl = clus.shape[0]
        deg = send.size // count
        memb = memb.reshape(count // TILE, TILE)
        gain = gain.reshape(1, width)
        args = (node, clus, send, memb, wk, wv, wei, weo, wni, wno, gain)
        peers = sum(n - 1 for n in sizes)
        total = ncl * (1 + peers)
        scratch = []
        for i, a in enumerate(args):
            space = pltpu.SMEM if i == 2 else pltpu.VMEM
            scratch.append(space(a.shape, a.dtype))
        scratch += [pltpu.VMEM(((n - 1) * ncl, width), BF16) for n in sizes]
        scratch += [
            pltpu.VMEM((6, BND, width), BF16),
            pltpu.VMEM((width, total), BF16),
            pltpu.VMEM((total, 2 * width), BF16),
            pltpu.VMEM((count + 6 * BND, width), F32),
            pltpu.VMEM((count, width), F32),
            pltpu.VMEM((deg, count, width), F32),
            pltpu.VMEM((count, 2 * width), F32),
            pltpu.VMEM((count, width), F32),
            pltpu.VMEM((count, width), F32),
            pltpu.VMEM((count, width), F32),
            pltpu.SemaphoreType.DMA((len(args),)),
            pltpu.SemaphoreType.DMA((peers,)),
            pltpu.SemaphoreType.DMA((peers,)),
            pltpu.SemaphoreType.DMA((6,)),
            pltpu.SemaphoreType.DMA((6,)),
            pltpu.SemaphoreType.DMA((2 * sizes[2],)),
            pltpu.SemaphoreType.DMA((sizes[2],)),
        ]
        return pl.pallas_call(
            functools.partial(kernel, sizes),
            out_shape=jax.ShapeDtypeStruct((count, width), BF16),
            in_specs=[pl.BlockSpec(memory_space=pltpu.HBM)] * len(args),
            out_specs=pl.BlockSpec(memory_space=pltpu.VMEM),
            scratch_shapes=scratch,
            compiler_params=pltpu.CompilerParams(
                collective_id=0, has_side_effects=True
            ),
        )(*args)

    spec = P(AXES, None)
    return jax.shard_map(
        on_device,
        mesh=mesh,
        in_specs=(spec, spec, spec, P(AXES)) + (P(),) * 7,
        out_specs=spec,
        check_vma=False,
    )
```
